32 devices in a mesh: keys: 8 (over z, y), view: 4 (over x, core).
Axes of the slice: x: 2, y: 2, z: 4, core: 2. Of those that a mesh axis runs over, the one named last changes fastest.
Arguments:
- key_slot: int32 [4096], replicated, may hold values from 0 to 4095, as said below
- a_slot: int32 [131072], P(('keys', 'view')), may hold values from 0 to 511
- a_group: int32 [131072], P(('keys', 'view')), may hold values from 0 to 1023
- a_weight: int32 [131072], P(('keys', 'view')), may hold values from 1 to 3
- a_payload: bfloat16 [131072, 256], P(('keys', 'view')), may hold values from -1.1953125 to 1.1953125
- b_slot: int32 [131072], P(('keys', 'view')), may hold values from 0 to 511
- b_weight: int32 [131072], P(('keys', 'view')), may hold values from 1 to 3
- b_payload: bfloat16 [131072, 256], P(('keys', 'view')), may hold values from -0.59765625 to 0.59765625
- da_key: int32 [32768], P(('keys', 'view')), may hold values from 0 to 4095, as said below
- da_group: int32 [32768], P(('keys', 'view')), may hold values from 0 to 1023
- da_mult: int32 [32768], P(('keys', 'view')), may hold values from -1 to 1, as said below
- da_payload: bfloat16 [32768, 256], P(('keys', 'view')), may hold values from -1.796875 to 1.796875
- da_count: int32 [32], P(('keys', 'view')), may hold values from 768 to 1024, as said below
- db_key: int32 [32768], P(('keys', 'view')), may hold values from 0 to 4095, as said below
- db_mult: int32 [32768], P(('keys', 'view')), may hold values from -1 to 1, as said below
- db_payload: bfloat16 [32768, 256], P(('keys', 'view')), may hold values from -1.1953125 to 1.1953125
- db_count: int32 [32], P(('keys', 'view')), may hold values from 768 to 1024, as said below
Outputs:
- view_delta: float32 [1024, 256], P(('keys', 'view'))
The draws below stay inside these ranges and needn't reach their ends.
Inputs may be any that keep to these rules, and one draw needn't show every extreme that they name: `key_slot`: A permutation of 0 to 4095. `da_key`: among the 1024 slots of one device, at most 256 have keys held by one keys index; in every draw one keys index gets exactly 256 live rows from every device. `db_key`: among the 1024 slots of one device, at most 256 have keys held by one keys index; in every draw one keys index gets exactly 256 live rows from every device. `da_mult`: each entry is -1 or 1. `db_mult`: each entry is -1 or 1. `da_count`: some device has all 1024 rows live. `db_count`: some device has all 1024 rows live.
All inputs are finite; a program needn't handle non-finite values.
Results may differ from the reference program's by a relative error of at most 0.0029.
Values may be sent and summed in bfloat16 or wider, within the bound.
A program may use at most 64 MiB of HBM per device.

```python
import jax
import jax.numpy as jnp

D = 256
KEYS_DEV = 512
GROUPS_DEV = 32
A_DEV = 4096
B_DEV = 4096
DELTA_DEV = 1024
CAP = 256
KEYS = 4096
GROUPS = 1024
A_ROWS = 131072
B_ROWS = 131072
DELTA_ROWS = 32768
N_KEYS = 8
N_VIEW = 4


def draw_key_slot(key, part):
    return jax.random.permutation(jax.random.fold_in(key, 11), KEYS).astype(jnp.int32)


def delta_keys(key, salt_value):
    order = draw_key_slot(key, 0)
    inverse = jnp.zeros((KEYS,), jnp.int32).at[order].set(jnp.arange(KEYS, dtype=jnp.int32))
    base = jax.random.fold_in(key, salt_value)
    hot_owner = jax.random.randint(jax.random.fold_in(base, 1), (), 0, N_KEYS).astype(jnp.int32)
    others = (hot_owner + 1 + jnp.arange(N_KEYS - 1, dtype=jnp.int32)) % N_KEYS
    target_pool = jnp.repeat(others, CAP, total_repeat_length=(N_KEYS - 1) * CAP)
    device_keys = jax.random.split(jax.random.fold_in(base, 2), N_KEYS * N_VIEW)

    def one_device(device_key):
        shuffled = jax.random.permutation(jax.random.fold_in(device_key, 3), target_pool)
        target = jnp.concatenate([jnp.full((CAP,), hot_owner, jnp.int32), shuffled[:DELTA_DEV - CAP]])
        within = jax.random.randint(jax.random.fold_in(device_key, 4), (DELTA_DEV,), 0, KEYS_DEV).astype(jnp.int32)
        return jnp.take(inverse, target * KEYS_DEV + within)
    return jax.vmap(one_device)(device_keys).reshape(-1).astype(jnp.int32)


def delta_signs(key, salt_value):
    picked = jax.random.randint(jax.random.fold_in(key, salt_value), (DELTA_ROWS,), 0, 2)
    return (2 * picked - 1).astype(jnp.int32)


def delta_counts(key, salt_value):
    devices = N_KEYS * N_VIEW
    counts = jax.random.randint(jax.random.fold_in(key, salt_value), (devices,), 3 * DELTA_DEV // 4, DELTA_DEV + 1)
    full_device = jax.random.randint(jax.random.fold_in(key, salt_value + 1), (), 0, devices)
    return counts.at[full_device].set(DELTA_DEV).astype(jnp.int32)


def draw_da_key(key, part):
    return delta_keys(key, 21)


def draw_db_key(key, part):
    return delta_keys(key, 22)


def draw_da_mult(key, part):
    return delta_signs(key, 31)


def draw_db_mult(key, part):
    return delta_signs(key, 32)


def draw_da_count(key, part):
    return delta_counts(key, 41)


def draw_db_count(key, part):
    return delta_counts(key, 51)


def plant(entries, own_key, smallest, high):
    dims = entries.shape
    place = [jax.random.randint(jax.random.fold_in(own_key, axis), (), 0, dims[axis]) for axis in range(len(dims))]
    entries = entries.at[tuple(place)].set(smallest)
    longest = dims.index(max(dims))
    place[longest] = (place[longest] + 1) % dims[longest]
    return entries.at[tuple(place)].set(high)


def block_scale(key, dims, pieces, least, high):
    gain = 1.0
    for axis_at, shards_of in pieces:
        heights = jax.random.uniform(jax.random.fold_in(jax.random.fold_in(key, 6), axis_at), (shards_of,), jnp.float32, least / len(pieces), high / len(pieces))
        gain = gain * jnp.repeat(jnp.exp(heights), dims[axis_at] // shards_of).reshape((-1,) + (1,) * (len(dims) - 1 - axis_at))
    return gain


def scatter_about(key, shape, width, bound, cuts=(), held_as=jnp.bfloat16):
    result = width * jax.random.normal(key, shape, jnp.float32)
    if cuts:
        result = result * block_scale(key, shape, cuts, -0.22, 0.18)
    return jnp.clip(result, -bound, bound).astype(held_as)


def setup_inputs(seed: int = 0) -> dict:
    splits = jax.random.split(jax.random.key(seed), 18)
    key_slot = draw_key_slot(jax.random.fold_in(splits[17], 71), 0)
    a_slot = plant(jax.random.randint(splits[1], (A_ROWS,), 0, KEYS_DEV), jax.random.fold_in(splits[1], 1), 0, KEYS_DEV - 1).astype(jnp.int32)
    a_group = plant(jax.random.randint(splits[2], (A_ROWS,), 0, GROUPS), jax.random.fold_in(splits[2], 1), 0, GROUPS - 1).astype(jnp.int32)
    a_weight = plant(jax.random.randint(splits[3], (A_ROWS,), 1, 4), jax.random.fold_in(splits[3], 1), 1, 3).astype(jnp.int32)
    a_payload = scatter_about(splits[4], (A_ROWS, D), 0.2, 1.1953125, ((0, 32),))
    b_slot = plant(jax.random.randint(splits[5], (B_ROWS,), 0, KEYS_DEV), jax.random.fold_in(splits[5], 1), 0, KEYS_DEV - 1).astype(jnp.int32)
    b_weight = plant(jax.random.randint(splits[6], (B_ROWS,), 1, 4), jax.random.fold_in(splits[6], 1), 1, 3).astype(jnp.int32)
    b_payload = scatter_about(splits[7], (B_ROWS, D), 0.1, 0.59765625, ((0, 32),))
    da_key = draw_da_key(jax.random.fold_in(splits[17], 71), 0)
    da_group = plant(jax.random.randint(splits[9], (DELTA_ROWS,), 0, GROUPS), jax.random.fold_in(splits[9], 1), 0, GROUPS - 1).astype(jnp.int32)
    da_mult = draw_da_mult(jax.random.fold_in(splits[17], 71), 0)
    da_payload = scatter_about(splits[11], (DELTA_ROWS, D), 0.3, 1.796875, ((0, 32),))
    da_count = draw_da_count(jax.random.fold_in(splits[17], 71), 0)
    db_key = draw_db_key(jax.random.fold_in(splits[17], 71), 0)
    db_mult = draw_db_mult(jax.random.fold_in(splits[17], 71), 0)
    db_payload = scatter_about(splits[15], (DELTA_ROWS, D), 0.2, 1.1953125, ((0, 32),))
    db_count = draw_db_count(jax.random.fold_in(splits[17], 71), 0)
    return dict(key_slot=key_slot, a_slot=a_slot, a_group=a_group, a_weight=a_weight, a_payload=a_payload, b_slot=b_slot, b_weight=b_weight, b_payload=b_payload, da_key=da_key, da_group=da_group, da_mult=da_mult, da_payload=da_payload, da_count=da_count, db_key=db_key, db_mult=db_mult, db_payload=db_payload, db_count=db_count)


def reference(key_slot, a_slot, a_group, a_weight, a_payload, b_slot, b_weight, b_payload, da_key, da_group, da_mult, da_payload, da_count, db_key, db_mult, db_payload, db_count):
    devices = N_KEYS * N_VIEW
    total_keys = KEYS_DEV * N_KEYS
    total_groups = GROUPS_DEV * devices

    def owner_slots(local_slot, rows_dev):
        device_index = jnp.arange(local_slot.shape[0], dtype=jnp.int32) // rows_dev
        return (device_index // N_VIEW) * KEYS_DEV + local_slot

    def signed_rows(row_mult, row_count):
        position = jnp.arange(DELTA_DEV * devices, dtype=jnp.int32)
        alive_rows = (position % DELTA_DEV) < jnp.take(row_count, position // DELTA_DEV)
        return (row_mult * alive_rows.astype(jnp.int32)).astype(jnp.float32)

    key_b = jax.ops.segment_sum(b_weight[:, None].astype(jnp.float32) * b_payload.astype(jnp.float32), owner_slots(b_slot, B_DEV), num_segments=total_keys)
    key_db = jax.ops.segment_sum(signed_rows(db_mult, db_count)[:, None] * db_payload.astype(jnp.float32), jnp.take(key_slot, db_key), num_segments=total_keys)
    a_terms = (a_weight[:, None].astype(jnp.float32) * a_payload.astype(jnp.float32) * jnp.take(key_db, owner_slots(a_slot, A_DEV), axis=0)).astype(jnp.bfloat16)
    whole_table = key_b + key_db
    delta_terms = (signed_rows(da_mult, da_count)[:, None] * da_payload.astype(jnp.float32) * jnp.take(whole_table, jnp.take(key_slot, da_key), axis=0)).astype(jnp.bfloat16)
    view_delta = jax.ops.segment_sum(a_terms.astype(jnp.float32), a_group, num_segments=total_groups)
    view_delta = view_delta + jax.ops.segment_sum(delta_terms.astype(jnp.float32), da_group, num_segments=total_groups)
    return view_delta
```

```python
import functools

import jax
import jax.numpy as jnp
from jax import lax
from jax.experimental import pallas as pl
from jax.experimental.pallas import tpu as pltpu
from jax.sharding import PartitionSpec as P

LANES = 128
META = 16
F32 = jnp.float32
BF16 = jnp.bfloat16
VMEM_LIMIT = 60 * 1024 * 1024


def row_of(ref, start, count):
    return jnp.concatenate([ref[pl.ds(start + i, 1), :] for i in range(count)], axis=1)


def as_row(ref):
    return row_of(ref, 0, ref.shape[0])


def iota(shape, axis):
    return lax.broadcasted_iota(jnp.int32, shape, axis)


def dot(a, b):
    return jnp.dot(a, b, preferred_element_type=F32)


def pack_side(owners, keys_dev, cap, base, table_ref, key_ref, mult_ref, group_ref, count, pay_ref, out_ref):
    rows = pay_ref.shape[0]
    tiles = table_ref.shape[0]
    key = as_row(key_ref)
    table = table_ref[...]
    halves = jnp.concatenate([table & 255, table >> 8], axis=0).astype(F32).astype(BF16)
    low = jnp.where(iota((LANES, rows), 0) == (key & (LANES - 1)), 1.0, 0.0).astype(BF16)
    looked = dot(halves, low)
    high = iota((tiles, rows), 0) == (key >> 7)
    slot_low = jnp.sum(jnp.where(high, looked[:tiles], 0.0), axis=0, keepdims=True)
    slot_high = jnp.sum(jnp.where(high, looked[tiles:], 0.0), axis=0, keepdims=True)
    slot = slot_low.astype(jnp.int32) + 256 * slot_high.astype(jnp.int32)
    owner = slot // keys_dev
    local = slot - owner * keys_dev
    alive = iota((1, rows), 1) < count
    marks = jnp.where((iota((owners, rows), 0) == owner) & alive, 1.0, 0.0)
    step = min(256, rows)
    upper = jnp.where(iota((step, step), 0) < iota((step, step), 1), 1.0, 0.0).astype(BF16)
    running = jnp.zeros((owners, 1), F32)
    ranks = []
    for at in range(0, rows, step):
        piece = marks[:, at:at + step]
        before = dot(piece.astype(BF16), upper) + running
        ranks.append(jnp.sum(piece * before, axis=0, keepdims=True))
        running = running + jnp.sum(piece, axis=1, keepdims=True)
    rank = jnp.concatenate(ranks, axis=1).astype(jnp.int32)
    dest = jnp.where(alive, owner * cap + rank, -1)
    sign = as_row(mult_ref).astype(F32)
    group = jnp.zeros((1, rows), jnp.int32) if group_ref is None else as_row(group_ref)
    parts = [local & 255, local >> 8, group & 255, group >> 8]
    meta = jnp.concatenate(
        [p.astype(F32) * sign for p in parts] + [jnp.zeros((META - 4, rows), F32)], axis=0
    ).astype(BF16)
    payload = pay_ref[...]

    def one(o, carry):
        place = jnp.where(iota((cap, rows), 0) == dest - o * cap, sign, 0.0).astype(BF16)
        out_ref[o, base:base + cap, :] = dot(place, payload).astype(BF16)
        columns = lax.dot_general(meta, place, (((1,), (1,)), ((), ())), preferred_element_type=F32)
        out_ref[o, base + cap:base + cap + META, :cap] = columns.astype(BF16)
        return carry

    lax.fori_loop(0, owners, one, 0)


def pack_kernel(owners, keys_dev, cap, a_count, b_count, table, a_key, a_group, a_mult, b_key, b_mult, a_pay, b_pay, out):
    pack_side(owners, keys_dev, cap, 0, table, a_key, a_mult, a_group, a_count[0], a_pay, out)
    pack_side(owners, keys_dev, cap, cap + META, table, b_key, b_mult, None, b_count[0], b_pay, out)


def meta_row(got, o, row, cap):
    low = got[o, row:row + 1, :cap].astype(F32)
    high = got[o, row + 1:row + 2, :cap].astype(F32)
    return low.astype(jnp.int32) + 256 * high.astype(jnp.int32)


def base_kernel(keys_dev, slot_ref, weight_ref, pay_ref, out_ref):
    chunk = min(1024, pay_ref.shape[0])
    lines = chunk // LANES
    out_ref[...] = jnp.zeros_like(out_ref)

    def one(c, carry):
        slot = row_of(slot_ref, c * lines, lines)
        weight = row_of(weight_ref, c * lines, lines).astype(F32)
        marks = jnp.where(iota((keys_dev, chunk), 0) == slot, weight, 0.0).astype(BF16)
        rows = pl.ds(pl.multiple_of(c * chunk, chunk), chunk)
        out_ref[...] += dot(marks, pay_ref[rows, :])
        return carry

    lax.fori_loop(0, pay_ref.shape[0] // chunk, one, 0)


def delta_kernel(keys_dev, cap, local_b, got, out_ref):
    base = cap + META
    width = local_b.shape[1]
    out_ref[:, :width] = local_b[...]
    out_ref[:, width:] = jnp.zeros_like(local_b)

    def one(o, carry):
        slot = meta_row(got, o, base + cap, cap)
        marks = jnp.where(iota((keys_dev, cap), 0) == slot, 1.0, 0.0).astype(BF16)
        out_ref[:, width:] += dot(marks, got[o, base:base + cap, :])
        return carry

    lax.fori_loop(0, got.shape[0], one, 0)


def split(x):
    top = x.astype(BF16)
    return jnp.concatenate([top, (x - top.astype(F32)).astype(BF16)], axis=1)


def columns_of(row, width):
    return jnp.transpose(jnp.broadcast_to(row, (width, row.shape[1])))


def gathered(row, weight, table, width):
    count, keys_dev = row.shape[1], table.shape[0]
    code = columns_of(row * 4 + weight, LANES)
    slot, scale = code >> 2, (code & 3).astype(F32)
    marks = jnp.concatenate(
        [
            jnp.where(iota((count, LANES), 1) + at == slot, scale, 0.0).astype(BF16)
            for at in range(0, keys_dev, LANES)
        ],
        axis=1,
    )
    both = dot(marks, table)
    return both[:, :width] + both[:, width:]


def terms_kernel(
    cap, a_slot, a_weight, a_group, a_pay, got, totals, out, a_table, d_table, a_terms, d_terms
):
    width = a_pay.shape[1]
    owners = got.shape[0]
    groups = out.shape[0]
    db = totals[:, width:]
    a_table[...] = split(db)
    d_table[...] = split(totals[:, :width] + db)
    chunk = min(256, a_pay.shape[0])
    lines = chunk // LANES

    def a_one(c, carry):
        rows = pl.ds(pl.multiple_of(c * chunk, chunk), chunk)
        picked = gathered(
            row_of(a_slot, c * lines, lines), row_of(a_weight, c * lines, lines), a_table[...], width
        )
        a_terms[rows, :] = (a_pay[rows, :].astype(F32) * picked).astype(BF16)
        return carry

    lax.fori_loop(0, a_pay.shape[0] // chunk, a_one, 0)

    def d_one(o, carry):
        slot = meta_row(got, o, cap, cap)
        picked = gathered(slot, jnp.ones_like(slot), d_table[...], width)
        d_terms[o] = (got[o, :cap, :].astype(F32) * picked).astype(BF16)
        return carry

    lax.fori_loop(0, owners, d_one, 0)

    block = min(256, groups)
    span = min(1024, a_pay.shape[0])
    span_lines = span // LANES

    def g_one(g, carry):
        first = g * block
        total = jnp.zeros((block, width), F32)
        ids = iota((block, 1), 0) + first
        for c in range(a_pay.shape[0] // span):
            group = row_of(a_group, c * span_lines, span_lines)
            marks = jnp.where(ids == group, 1.0, 0.0).astype(BF16)
            total = total + dot(marks, a_terms[c * span:(c + 1) * span, :])
        for o in range(owners):
            group = meta_row(got, o, cap + 2, cap)
            marks = jnp.where(ids == group, 1.0, 0.0).astype(BF16)
            total = total + dot(marks, d_terms[o])
        out[pl.ds(pl.multiple_of(first, block), block), :] = total.astype(BF16)
        return carry

    lax.fori_loop(0, groups // block, g_one, 0)


def call(body, shape, dtype, scratch=(), smem=0):
    def run(*args):
        specs = [pl.BlockSpec(memory_space=pltpu.SMEM)] * smem + [
            pl.BlockSpec(memory_space=pltpu.VMEM)
        ] * (len(args) - smem)
        return pl.pallas_call(
            body,
            out_shape=jax.ShapeDtypeStruct(shape, dtype),
            in_specs=specs,
            out_specs=pl.BlockSpec(memory_space=pltpu.VMEM),
            scratch_shapes=list(scratch),
            compiler_params=pltpu.CompilerParams(vmem_limit_bytes=VMEM_LIMIT),
        )(*args)

    return run


def view_total(x, views):
    me = lax.axis_index("view")
    trail = []
    bit = 1
    while bit < views:
        pairs = [(i, i ^ bit) for i in range(views)]
        if bit * 2 < views:
            mine = (me // bit) % 2
            half = x.shape[0] // 2
            keep = lax.dynamic_slice_in_dim(x, mine * half, half, 0)
            give = lax.dynamic_slice_in_dim(x, (1 - mine) * half, half, 0)
            x = keep + lax.ppermute(give, "view", pairs)
            trail.append((pairs, mine))
        else:
            x = x + lax.ppermute(x, "view", pairs)
        bit *= 2
    for pairs, mine in reversed(trail):
        other = lax.ppermute(x, "view", pairs)
        x = jnp.where(mine == 0, jnp.concatenate([x, other]), jnp.concatenate([other, x]))
    return x


def shards(
    keys_total, key_slot, a_slot, a_group, a_weight, a_payload, b_slot, b_weight, b_payload,
    da_key, da_group, da_mult, da_payload, da_count, db_key, db_mult, db_payload, db_count,
):
    owners, views = lax.axis_size("keys"), lax.axis_size("view")
    devices = owners * views
    width = a_payload.shape[1]
    keys_dev = key_slot.shape[0] // owners
    delta = da_payload.shape[0]
    cap = 2 * delta // owners
    groups = keys_total

    def lined(x):
        return x.reshape(-1, LANES)

    sent = call(
        functools.partial(pack_kernel, owners, keys_dev, cap), (owners, 2 * (cap + META), width), BF16, smem=2
    )(
        da_count, db_count, lined(key_slot), lined(da_key), lined(da_group), lined(da_mult),
        lined(db_key), lined(db_mult), da_payload, db_payload,
    )
    got = lax.all_to_all(sent, "keys", split_axis=0, concat_axis=0, tiled=True)
    local_b = call(functools.partial(base_kernel, keys_dev), (keys_dev, width), F32)(
        lined(b_slot), lined(b_weight), b_payload
    )
    local = call(functools.partial(delta_kernel, keys_dev, cap), (keys_dev, 2 * width), F32)(local_b, got)
    totals = view_total(local, views)
    summed = call(
        functools.partial(terms_kernel, cap),
        (groups, width),
        BF16,
        scratch=[
            pltpu.VMEM((keys_dev, 2 * width), BF16),
            pltpu.VMEM((keys_dev, 2 * width), BF16),
            pltpu.VMEM(a_payload.shape, BF16),
            pltpu.VMEM((owners, cap, width), BF16),
        ],
    )(
        lined(a_slot), lined(a_weight), lined(a_group), a_payload, got, totals
    )
    pieces = lax.all_to_all(
        summed.reshape(devices, groups // devices, width), ("keys", "view"), split_axis=0, concat_axis=0, tiled=True
    )
    return jnp.sum(pieces.astype(F32), axis=0)


GROUPS_DEV = 32


def solution(mesh):
    row, wide = P(("keys", "view")), P(("keys", "view"), None)
    groups = GROUPS_DEV * mesh.shape["keys"] * mesh.shape["view"]
    in_specs = (P(), row, row, row, wide, row, row, wide, row, row, row, wide, row, row, row, wide, row)
    return jax.shard_map(
        functools.partial(shards, groups), mesh=mesh, in_specs=in_specs, out_specs=wide, check_vma=False
    )
```

```python
import functools

import jax
import jax.numpy as jnp
from jax import lax
from jax.experimental import pallas as pl
from jax.experimental.pallas import tpu as pltpu
from jax.sharding import PartitionSpec as P


LANES = 128
META = 16
F32 = jnp.float32
BF16 = jnp.bfloat16
VMEM_LIMIT = 20 * 1024 * 1024


def row_of(ref, start, count):
    return jnp.concatenate([ref[pl.ds(start + i, 1), :] for i in range(count)], axis=1)


def as_row(ref):
    return row_of(ref, 0, ref.shape[0])


def iota(shape, axis):
    return lax.broadcasted_iota(jnp.int32, shape, axis)


def dot(a, b):
    return jnp.dot(a, b, preferred_element_type=F32)


def pack_side(owners, keys_dev, cap, base, table_ref, key_ref, mult_ref, group_ref, count, pay_ref, out_ref):
    rows = pay_ref.shape[0]
    tiles = table_ref.shape[0]
    key = as_row(key_ref)
    table = table_ref[...]
    halves = jnp.concatenate([table & 255, table >> 8], axis=0).astype(F32).astype(BF16)
    low = jnp.where(iota((LANES, rows), 0) == (key & (LANES - 1)), 1.0, 0.0).astype(BF16)
    looked = dot(halves, low)
    high = iota((tiles, rows), 0) == (key >> 7)
    slot_low = jnp.sum(jnp.where(high, looked[:tiles], 0.0), axis=0, keepdims=True)
    slot_high = jnp.sum(jnp.where(high, looked[tiles:], 0.0), axis=0, keepdims=True)
    slot = slot_low.astype(jnp.int32) + 256 * slot_high.astype(jnp.int32)
    owner = slot // keys_dev
    local = slot - owner * keys_dev
    alive = iota((1, rows), 1) < count
    marks = jnp.where((iota((owners, rows), 0) == owner) & alive, 1.0, 0.0)
    step = min(256, rows)
    upper = jnp.where(iota((step, step), 0) < iota((step, step), 1), 1.0, 0.0).astype(BF16)
    running = jnp.zeros((owners, 1), F32)
    ranks = []
    for at in range(0, rows, step):
        piece = marks[:, at:at + step]
        before = dot(piece.astype(BF16), upper) + running
        ranks.append(jnp.sum(piece * before, axis=0, keepdims=True))
        running = running + jnp.sum(piece, axis=1, keepdims=True)
    rank = jnp.concatenate(ranks, axis=1).astype(jnp.int32)
    dest = jnp.where(alive, owner * cap + rank, -1)
    sign = as_row(mult_ref).astype(F32)
    group = jnp.zeros((1, rows), jnp.int32) if group_ref is None else as_row(group_ref)
    parts = [local & 255, local >> 8, group & 255, group >> 8]
    meta = jnp.concatenate(
        [p.astype(F32) * sign for p in parts] + [jnp.zeros((META - 4, rows), F32)], axis=0
    ).astype(BF16)
    payload = pay_ref[...]

    def one(o, carry):
        place = jnp.where(iota((cap, rows), 0) == dest - o * cap, sign, 0.0).astype(BF16)
        out_ref[o, base:base + cap, :] = dot(place, payload).astype(BF16)
        columns = lax.dot_general(meta, place, (((1,), (1,)), ((), ())), preferred_element_type=F32)
        out_ref[o, base + cap:base + cap + META, :cap] = columns.astype(BF16)
        return carry

    lax.fori_loop(0, owners, one, 0)


def pack_a_kernel(owners, keys_dev, cap, count, table, key, group, mult, pay, out):
    pack_side(owners, keys_dev, cap, 0, table, key, mult, group, count[0], pay, out)


def pack_b_kernel(owners, keys_dev, cap, count, table, key, mult, pay, out):
    pack_side(owners, keys_dev, cap, 0, table, key, mult, None, count[0], pay, out)


def meta_row(got, o, row, cap):
    low = got[o, row:row + 1, :cap].astype(F32)
    high = got[o, row + 1:row + 2, :cap].astype(F32)
    return low.astype(jnp.int32) + 256 * high.astype(jnp.int32)


def base_kernel(keys_dev, slot_ref, weight_ref, pay_ref, out_ref):
    chunk = min(1024, pay_ref.shape[0])
    lines = chunk // LANES
    out_ref[...] = jnp.zeros_like(out_ref)

    def one(c, carry):
        slot = row_of(slot_ref, c * lines, lines)
        weight = row_of(weight_ref, c * lines, lines).astype(F32)
        marks = jnp.where(iota((keys_dev, chunk), 0) == slot, weight, 0.0).astype(BF16)
        rows = pl.ds(pl.multiple_of(c * chunk, chunk), chunk)
        out_ref[...] += dot(marks, pay_ref[rows, :])
        return carry

    lax.fori_loop(0, pay_ref.shape[0] // chunk, one, 0)


def delta_kernel(keys_dev, cap, got, out_ref):
    out_ref[...] = jnp.zeros_like(out_ref)

    def one(o, carry):
        slot = meta_row(got, o, cap, cap)
        marks = jnp.where(iota((keys_dev, cap), 0) == slot, 1.0, 0.0).astype(BF16)
        out_ref[...] += dot(marks, got[o, :cap, :])
        return carry

    lax.fori_loop(0, got.shape[0], one, 0)


def split(x):
    top = x.astype(BF16)
    return jnp.concatenate([top, (x - top.astype(F32)).astype(BF16)], axis=1)


def columns_of(row, width):
    return jnp.transpose(jnp.broadcast_to(row, (width, row.shape[1])))


def gathered(row, weight, table, width):
    count, keys_dev = row.shape[1], table.shape[0]
    code = columns_of(row * 4 + weight, LANES)
    slot, scale = code >> 2, (code & 3).astype(F32)
    marks = jnp.concatenate(
        [
            jnp.where(iota((count, LANES), 1) + at == slot, scale, 0.0).astype(BF16)
            for at in range(0, keys_dev, LANES)
        ],
        axis=1,
    )
    both = dot(marks, table)
    return both[:, :width] + both[:, width:]


def a_kernel(a_slot, a_weight, a_group, a_pay, db, out, table, terms):
    count, width = a_pay.shape
    groups = out.shape[0]
    table[...] = split(db[...])
    chunk = min(256, count)
    lines = chunk // LANES

    def one(c, carry):
        rows = pl.ds(pl.multiple_of(c * chunk, chunk), chunk)
        picked = gathered(
            row_of(a_slot, c * lines, lines), row_of(a_weight, c * lines, lines), table[...], width
        )
        terms[rows, :] = (a_pay[rows, :].astype(F32) * picked).astype(BF16)
        return carry

    lax.fori_loop(0, count // chunk, one, 0)

    block = min(256, groups)
    span = min(1024, count)
    span_lines = span // LANES

    def g_one(g, carry):
        first = g * block
        total = jnp.zeros((block, width), F32)
        ids = iota((block, 1), 0) + first
        for c in range(count // span):
            group = row_of(a_group, c * span_lines, span_lines)
            marks = jnp.where(ids == group, 1.0, 0.0).astype(BF16)
            total = total + dot(marks, terms[c * span:(c + 1) * span, :])
        out[pl.ds(pl.multiple_of(first, block), block), :] = total
        return carry

    lax.fori_loop(0, groups // block, g_one, 0)


def d_kernel(cap, got, b, db, partial, out, table, terms):
    owners, _, width = got.shape
    groups = out.shape[0]
    table[...] = split(b[...] + db[...])

    def one(o, carry):
        slot = meta_row(got, o, cap, cap)
        picked = gathered(slot, jnp.ones_like(slot), table[...], width)
        terms[o] = (got[o, :cap, :].astype(F32) * picked).astype(BF16)
        return carry

    lax.fori_loop(0, owners, one, 0)
    block = min(256, groups)

    def g_one(g, carry):
        first = g * block
        rows = pl.ds(pl.multiple_of(first, block), block)
        total = partial[rows, :]
        ids = iota((block, 1), 0) + first
        for o in range(owners):
            group = meta_row(got, o, cap + 2, cap)
            marks = jnp.where(ids == group, 1.0, 0.0).astype(BF16)
            total = total + dot(marks, terms[o])
        out[rows, :] = total.astype(BF16)
        return carry

    lax.fori_loop(0, groups // block, g_one, 0)


def call(body, shape, dtype, flops, scratch=(), smem=0):
    def run(*args):
        specs = [pl.BlockSpec(memory_space=pltpu.SMEM)] * smem + [
            pl.BlockSpec(memory_space=pltpu.VMEM)
        ] * (len(args) - smem)
        return pl.pallas_call(
            body,
            out_shape=jax.ShapeDtypeStruct(shape, dtype),
            in_specs=specs,
            out_specs=pl.BlockSpec(memory_space=pltpu.VMEM),
            scratch_shapes=list(scratch),
            compiler_params=pltpu.CompilerParams(vmem_limit_bytes=VMEM_LIMIT),
            cost_estimate=pl.CostEstimate(
                flops=4 * flops, bytes_accessed=sum(x.size * x.dtype.itemsize for x in args), transcendentals=0
            ),
        )(*args)

    return run


def view_total(x, views):
    me = lax.axis_index("view")
    trail = []
    bit = 1
    while bit < views:
        pairs = [(i, i ^ bit) for i in range(views)]
        if bit * 2 < views:
            mine = (me // bit) % 2
            half = x.shape[0] // 2
            keep = lax.dynamic_slice_in_dim(x, mine * half, half, 0)
            give = lax.dynamic_slice_in_dim(x, (1 - mine) * half, half, 0)
            x = keep + lax.ppermute(give, "view", pairs)
            trail.append((pairs, mine))
        else:
            x = x + lax.ppermute(x, "view", pairs)
        bit *= 2
    for pairs, mine in reversed(trail):
        other = lax.ppermute(x, "view", pairs)
        x = jnp.where(mine == 0, jnp.concatenate([x, other]), jnp.concatenate([other, x]))
    return x


def shards(
    keys_total, key_slot, a_slot, a_group, a_weight, a_payload, b_slot, b_weight, b_payload,
    da_key, da_group, da_mult, da_payload, da_count, db_key, db_mult, db_payload, db_count,
):
    owners, views = lax.axis_size("keys"), lax.axis_size("view")
    devices = owners * views
    width = a_payload.shape[1]
    keys_dev = key_slot.shape[0] // owners
    delta = da_payload.shape[0]
    cap = 2 * delta // owners
    groups = keys_total

    def lined(x):
        return x.reshape(-1, LANES)

    packed = (owners, cap + META, width)
    pack_flops = 2 * owners * cap * delta * width
    b_sent = call(functools.partial(pack_b_kernel, owners, keys_dev, cap), packed, BF16, pack_flops, smem=1)(
        db_count, lined(key_slot), lined(db_key), lined(db_mult), db_payload
    )
    b_got = lax.all_to_all(b_sent, "keys", split_axis=0, concat_axis=0, tiled=True)
    a_sent = call(functools.partial(pack_a_kernel, owners, keys_dev, cap), packed, BF16, pack_flops, smem=1)(
        da_count, lined(key_slot), lined(da_key), lined(da_group), lined(da_mult), da_payload
    )
    local_b = call(
        functools.partial(base_kernel, keys_dev), (keys_dev, width), F32, 2 * keys_dev * b_payload.size
    )(lined(b_slot), lined(b_weight), b_payload)
    total_b = view_total(local_b, views)
    b_got, a_sent, total_b = lax.optimization_barrier((b_got, a_sent, total_b))
    a_got = lax.all_to_all(a_sent, "keys", split_axis=0, concat_axis=0, tiled=True)
    local_db = call(
        functools.partial(delta_kernel, keys_dev, cap), (keys_dev, width), F32, 2 * keys_dev * owners * cap * width
    )(b_got)
    total_db = view_total(local_db, views)
    table = pltpu.VMEM((keys_dev, 2 * width), BF16)
    a_flops = (4 * keys_dev + 2 * groups) * a_payload.size
    partial = call(
        a_kernel, (groups, width), F32, a_flops, scratch=[table, pltpu.VMEM(a_payload.shape, BF16)]
    )(lined(a_slot), lined(a_weight), lined(a_group), a_payload, total_db)
    summed = call(
        functools.partial(d_kernel, cap),
        (groups, width),
        BF16,
        (4 * keys_dev + 2 * groups) * owners * cap * width,
        scratch=[table, pltpu.VMEM((owners, cap, width), BF16)],
    )(a_got, total_b, total_db, partial)
    pieces = lax.all_to_all(
        summed.reshape(devices, groups // devices, width), ("keys", "view"), split_axis=0, concat_axis=0, tiled=True
    )
    return jnp.sum(pieces.astype(F32), axis=0)


GROUPS_DEV = 32


def solution(mesh):
    row, wide = P(("keys", "view")), P(("keys", "view"), None)
    groups = GROUPS_DEV * mesh.shape["keys"] * mesh.shape["view"]
    in_specs = (P(), row, row, row, wide, row, row, wide, row, row, row, wide, row, row, row, wide, row)
    return jax.shard_map(
        functools.partial(shards, groups), mesh=mesh, in_specs=in_specs, out_specs=wide, check_vma=False
    )
```

```python
import functools

import jax
import jax.numpy as jnp
from jax import lax
from jax.experimental import pallas as pl
from jax.experimental.pallas import tpu as pltpu
from jax.sharding import PartitionSpec as P


LANES = 128
META = 8
F32 = jnp.float32
BF16 = jnp.bfloat16
VMEM_LIMIT = 16 * 1024 * 1024
WHOLE_LIMIT = 60 * 1024 * 1024


def row_of(ref, start, count):
    return jnp.concatenate([ref[pl.ds(start + i, 1), :] for i in range(count)], axis=1)


def as_row(ref):
    return row_of(ref, 0, ref.shape[0])


def iota(shape, axis):
    return lax.broadcasted_iota(jnp.int32, shape, axis)


def dot(a, b):
    return jnp.dot(a, b, preferred_element_type=F32)


def pack_side(owners, keys_dev, cap, base, table_ref, key_ref, mult_ref, group_ref, count, pay_ref, out_ref):
    rows = pay_ref.shape[0]
    tiles = table_ref.shape[0]
    key = as_row(key_ref)
    table = table_ref[...]
    halves = jnp.concatenate([table & 255, table >> 8], axis=0).astype(F32).astype(BF16)
    low = jnp.where(iota((LANES, rows), 0) == (key & (LANES - 1)), 1.0, 0.0).astype(BF16)
    looked = dot(halves, low)
    high = iota((tiles, rows), 0) == (key >> 7)
    slot_low = jnp.sum(jnp.where(high, looked[:tiles], 0.0), axis=0, keepdims=True)
    slot_high = jnp.sum(jnp.where(high, looked[tiles:], 0.0), axis=0, keepdims=True)
    slot = slot_low.astype(jnp.int32) + 256 * slot_high.astype(jnp.int32)
    owner = slot // keys_dev
    local = slot - owner * keys_dev
    alive = iota((1, rows), 1) < count
    marks = jnp.where((iota((owners, rows), 0) == owner) & alive, 1.0, 0.0)
    step = min(256, rows)
    upper = jnp.where(iota((step, step), 0) < iota((step, step), 1), 1.0, 0.0).astype(BF16)
    running = jnp.zeros((owners, 1), F32)
    ranks = []
    for at in range(0, rows, step):
        piece = marks[:, at:at + step]
        before = dot(piece.astype(BF16), upper) + running
        ranks.append(jnp.sum(piece * before, axis=0, keepdims=True))
        running = running + jnp.sum(piece, axis=1, keepdims=True)
    rank = jnp.concatenate(ranks, axis=1).astype(jnp.int32)
    dest = jnp.where(alive, owner * cap + rank, -1)
    sign = as_row(mult_ref).astype(F32)
    group = jnp.zeros((1, rows), jnp.int32) if group_ref is None else as_row(group_ref)
    parts = [local & 255, local >> 8, group & 255, group >> 8]
    meta = jnp.concatenate(
        [p.astype(F32) * sign for p in parts] + [jnp.zeros((META - 4, rows), F32)], axis=0
    ).astype(BF16)
    payload = pay_ref[...]

    def one(o, carry):
        place = jnp.where(iota((cap, rows), 0) == dest - o * cap, sign, 0.0).astype(BF16)
        out_ref[o, base:base + cap, :] = dot(place, payload).astype(BF16)
        columns = lax.dot_general(meta, place, (((1,), (1,)), ((), ())), preferred_element_type=F32)
        out_ref[o, base + cap:base + cap + META, :cap] = columns.astype(BF16)
        return carry

    lax.fori_loop(0, owners, one, 0)


def pack_a_kernel(owners, keys_dev, cap, count, table, key, group, mult, pay, out):
    pack_side(owners, keys_dev, cap, 0, table, key, mult, group, count[0], pay, out)


def pack_b_kernel(owners, keys_dev, cap, count, table, key, mult, pay, out):
    pack_side(owners, keys_dev, cap, 0, table, key, mult, None, count[0], pay, out)


def meta_row(got, o, row, cap):
    low = got[o, row:row + 1, :cap].astype(F32)
    high = got[o, row + 1:row + 2, :cap].astype(F32)
    return low.astype(jnp.int32) + 256 * high.astype(jnp.int32)


def base_kernel(keys_dev, slot_ref, weight_ref, pay_ref, out_ref):
    chunk = min(1024, pay_ref.shape[0])
    lines = chunk // LANES
    out_ref[...] = jnp.zeros_like(out_ref)

    def one(c, carry):
        slot = row_of(slot_ref, c * lines, lines)
        weight = row_of(weight_ref, c * lines, lines).astype(F32)
        marks = jnp.where(iota((keys_dev, chunk), 0) == slot, weight, 0.0).astype(BF16)
        rows = pl.ds(pl.multiple_of(c * chunk, chunk), chunk)
        out_ref[...] += dot(marks, pay_ref[rows, :])
        return carry

    lax.fori_loop(0, pay_ref.shape[0] // chunk, one, 0)


def delta_kernel(keys_dev, cap, got, out_ref):
    out_ref[...] = jnp.zeros_like(out_ref)

    def one(o, carry):
        slot = meta_row(got, o, cap, cap)
        marks = jnp.where(iota((keys_dev, cap), 0) == slot, 1.0, 0.0).astype(BF16)
        out_ref[...] += dot(marks, got[o, :cap, :])
        return carry

    lax.fori_loop(0, got.shape[0], one, 0)


def split(x):
    top = x.astype(BF16)
    return jnp.concatenate([top, (x - top.astype(F32)).astype(BF16)], axis=1)


def columns_of(row, width):
    return jnp.transpose(jnp.broadcast_to(row, (width, row.shape[1])))


def gathered(row, weight, table, width):
    count, keys_dev = row.shape[1], table.shape[0]
    code = columns_of(row * 4 + weight, LANES)
    slot, scale = code >> 2, (code & 3).astype(F32)
    marks = jnp.concatenate(
        [
            jnp.where(iota((count, LANES), 1) + at == slot, scale, 0.0).astype(BF16)
            for at in range(0, keys_dev, LANES)
        ],
        axis=1,
    )
    both = dot(marks, table)
    return both[:, :width] + both[:, width:]


def group_ids(first, block, groups, owners, views):
    per_view = groups // views
    held = per_view // owners
    place = first // per_view
    at = iota((block, 1), 0) + (first - place * per_view)
    bits = views.bit_length() - 1
    rel = sum(((place >> b) & 1) << (bits - 1 - b) for b in range(bits))
    view = rel ^ lax.axis_index("view")
    owner = at // held
    return (owner * views + view) * held + (at - owner * held)


def a_kernel(owners, views, a_slot, a_weight, a_group, a_pay, db, out, table, terms):
    count, width = a_pay.shape
    groups = out.shape[0]
    table[...] = split(db[...])
    chunk = min(256, count)
    lines = chunk // LANES

    def one(c, carry):
        rows = pl.ds(pl.multiple_of(c * chunk, chunk), chunk)
        picked = gathered(
            row_of(a_slot, c * lines, lines), row_of(a_weight, c * lines, lines), table[...], width
        )
        terms[rows, :] = (a_pay[rows, :].astype(F32) * picked).astype(BF16)
        return carry

    lax.fori_loop(0, count // chunk, one, 0)

    block = min(256, groups // views)
    span = min(1024, count)
    span_lines = span // LANES

    def g_one(g, carry):
        first = g * block
        total = jnp.zeros((block, width), F32)
        ids = group_ids(first, block, groups, owners, views)
        for c in range(count // span):
            group = row_of(a_group, c * span_lines, span_lines)
            marks = jnp.where(ids == group, 1.0, 0.0).astype(BF16)
            total = total + dot(marks, terms[c * span:(c + 1) * span, :])
        out[pl.ds(pl.multiple_of(first, block), block), :] = total
        return carry

    lax.fori_loop(0, groups // block, g_one, 0)


def d_kernel(cap, views, got, b, db, partial, keep, give, table, terms):
    owners, _, width = got.shape
    groups = partial.shape[0]
    table[...] = split(b[...] + db[...])

    def one(o, carry):
        slot = meta_row(got, o, cap, cap)
        picked = gathered(slot, jnp.ones_like(slot), table[...], width)
        terms[o] = (got[o, :cap, :].astype(F32) * picked).astype(BF16)
        return carry

    lax.fori_loop(0, owners, one, 0)
    block = min(256, groups // views)

    def g_one(g):
        first = g * block
        rows = pl.ds(pl.multiple_of(first, block), block)
        total = partial[rows, :]
        ids = group_ids(first, block, groups, owners, views)
        for o in range(owners):
            group = meta_row(got, o, cap + 2, cap)
            marks = jnp.where(ids == group, 1.0, 0.0).astype(BF16)
            total = total + dot(marks, terms[o])
        return first, total

    def k_one(g, carry):
        first, total = g_one(g)
        keep[pl.ds(pl.multiple_of(first, block), block), :] = total
        return carry

    def s_one(g, carry):
        first, total = g_one(g + blocks)
        give[pl.ds(pl.multiple_of(first - groups // 2, block), block), :] = total
        return carry

    blocks = groups // 2 // block
    lax.fori_loop(0, blocks, s_one, 0)
    lax.fori_loop(0, blocks, k_one, 0)


def call(body, shape, dtype, flops, scratch=(), smem=0, outs=1, limit=VMEM_LIMIT):
    def run(*args):
        specs = [pl.BlockSpec(memory_space=pltpu.SMEM)] * smem + [
            pl.BlockSpec(memory_space=pltpu.VMEM)
        ] * (len(args) - smem)
        made = pl.pallas_call(
            body,
            out_shape=[jax.ShapeDtypeStruct(shape, dtype)] * outs,
            in_specs=specs,
            out_specs=[pl.BlockSpec(memory_space=pltpu.VMEM)] * outs,
            scratch_shapes=list(scratch),
            compiler_params=pltpu.CompilerParams(vmem_limit_bytes=limit),
            cost_estimate=pl.CostEstimate(
                flops=4 * flops, bytes_accessed=sum(x.size * x.dtype.itemsize for x in args), transcendentals=0
            ),
        )(*args)
        return made if outs > 1 else made[0]

    return run


def view_total(x, views):
    me = lax.axis_index("view")
    trail = []
    bit = 1
    while bit < views:
        pairs = [(i, i ^ bit) for i in range(views)]
        if bit * 2 < views:
            mine = (me // bit) % 2
            half = x.shape[0] // 2
            keep = lax.dynamic_slice_in_dim(x, mine * half, half, 0)
            give = lax.dynamic_slice_in_dim(x, (1 - mine) * half, half, 0)
            x = keep + lax.ppermute(give, "view", pairs)
            trail.append((pairs, mine))
        else:
            x = x + lax.ppermute(x, "view", pairs)
        bit *= 2
    for pairs, mine in reversed(trail):
        other = lax.ppermute(x, "view", pairs)
        x = jnp.where(mine == 0, jnp.concatenate([x, other]), jnp.concatenate([other, x]))
    return x


def shards(
    keys_total, key_slot, a_slot, a_group, a_weight, a_payload, b_slot, b_weight, b_payload,
    da_key, da_group, da_mult, da_payload, da_count, db_key, db_mult, db_payload, db_count,
):
    owners, views = lax.axis_size("keys"), lax.axis_size("view")
    width = a_payload.shape[1]
    keys_dev = key_slot.shape[0] // owners
    delta = da_payload.shape[0]
    cap = 2 * delta // owners
    groups = keys_total

    def lined(x):
        return x.reshape(-1, LANES)

    packed = (owners, cap + META, width)
    pack_flops = 2 * owners * cap * delta * width
    b_sent = call(functools.partial(pack_b_kernel, owners, keys_dev, cap), packed, BF16, pack_flops, smem=1, limit=WHOLE_LIMIT)(
        db_count, lined(key_slot), lined(db_key), lined(db_mult), db_payload
    )
    b_got = lax.all_to_all(b_sent, "keys", split_axis=0, concat_axis=0, tiled=True)
    a_sent = call(functools.partial(pack_a_kernel, owners, keys_dev, cap), packed, BF16, pack_flops, smem=1)(
        da_count, lined(key_slot), lined(da_key), lined(da_group), lined(da_mult), da_payload
    )
    local_b = call(
        functools.partial(base_kernel, keys_dev), (keys_dev, width), F32, 2 * keys_dev * b_payload.size
    )(lined(b_slot), lined(b_weight), b_payload)
    total_b = view_total(local_b, views)
    b_got, a_sent, total_b = lax.optimization_barrier((b_got, a_sent, total_b))
    a_got = lax.all_to_all(a_sent, "keys", split_axis=0, concat_axis=0, tiled=True)
    local_db = call(
        functools.partial(delta_kernel, keys_dev, cap), (keys_dev, width), F32, 2 * keys_dev * owners * cap * width
    )(b_got)
    total_db = view_total(local_db, views)
    table = pltpu.VMEM((keys_dev, 2 * width), BF16)
    a_flops = (4 * keys_dev + 2 * groups) * a_payload.size
    partial = call(
        functools.partial(a_kernel, owners, views), (groups, width), F32, a_flops, scratch=[table, pltpu.VMEM(a_payload.shape, BF16)]
    )(lined(a_slot), lined(a_weight), lined(a_group), a_payload, total_db)
    keep, give = call(
        functools.partial(d_kernel, cap, views),
        (groups // 2, width),
        F32,
        (4 * keys_dev + 2 * groups) * owners * cap * width,
        scratch=[table, pltpu.VMEM((owners, cap, width), BF16)],
        outs=2,
    )(a_got, total_b, total_db, partial)
    total = keep + lax.ppermute(give, "view", [(i, i ^ 1) for i in range(views)])
    bit = 2
    while bit < views:
        half = total.shape[0] // 2
        given = total[half:].astype(BF16)
        total = total[:half] + lax.ppermute(given, "view", [(i, i ^ bit) for i in range(views)]).astype(F32)
        bit *= 2
    pieces = lax.all_to_all(
        total.astype(BF16).reshape(owners, -1, width), "keys", split_axis=0, concat_axis=0, tiled=True
    )
    return jnp.sum(pieces.astype(F32), axis=0)


GROUPS_DEV = 32


def solution(mesh):
    row, wide = P(("keys", "view")), P(("keys", "view"), None)
    groups = GROUPS_DEV * mesh.shape["keys"] * mesh.shape["view"]
    in_specs = (P(), row, row, row, wide, row, row, wide, row, row, row, wide, row, row, row, wide, row)
    return jax.shard_map(
        functools.partial(shards, groups), mesh=mesh, in_specs=in_specs, out_specs=wide, check_vma=False
    )
```
